8 devices in a mesh: dp: 1 (over z), tp: 2 (over y), ep: 4 (over x, core).
Axes of the slice: x: 2, y: 2, z: 1, core: 2. Of those that a mesh axis runs over, the one named last changes fastest.
Arguments:
- hidden: bfloat16 [256, 2048], P(('dp', 'ep'))
- seq_lens: int32 [256], P(('dp', 'ep'))
- rope_cos: float32 [256, 64], P(('dp', 'ep'))
- rope_sin: float32 [256, 64], P(('dp', 'ep'))
- ln1_scale: bfloat16 [2048], replicated
- ln1_bias: bfloat16 [2048], replicated
- w_qkv: bfloat16 [2048, 5120], P(None, 'tp')
- b_qkv: bfloat16 [5120], P('tp')
- w_out: bfloat16 [4096, 2048], P('tp')
- b_out: bfloat16 [2048], replicated
- k_cache: bfloat16 [256, 128, 4, 128], P(('dp', 'ep'), None, 'tp')
- v_cache: bfloat16 [256, 128, 4, 128], P(('dp', 'ep'), None, 'tp')
- ln2_scale: bfloat16 [2048], replicated
- ln2_bias: bfloat16 [2048], replicated
- w_router: bfloat16 [2048, 128], replicated
- expert_ids: int32 [256, 8], P(('dp', 'ep'))
- w_gate: bfloat16 [128, 2048, 768], P('ep', None, 'tp')
- w_up: bfloat16 [128, 2048, 768], P('ep', None, 'tp')
- w_down: bfloat16 [128, 768, 2048], P('ep', 'tp')
Outputs:
- output 1: bfloat16 [256, 2048], P(('dp', 'ep'))
- output 2: bfloat16 [256, 128, 4, 128], P(('dp', 'ep'), None, 'tp')
- output 3: bfloat16 [256, 128, 4, 128], P(('dp', 'ep'), None, 'tp')
All inputs are finite; a program needn't handle non-finite values.
Results may differ from the reference program's by a relative error of at most 0.0107399.
Values are sent between devices in bfloat16 or wider.
A program may use at most 1 GiB of HBM per device.

```python
import jax
import jax.numpy as jnp
from jax import lax

D = 2048
HEADS = 32
KV_HEADS = 4
HEAD = 128
EXPERTS = 128
TOP = 8
FF = 768
BATCH = 64
SMAX = 128
EP_SHARDS = 4

TOKENS = EP_SHARDS * BATCH
Q_PER_GROUP = HEADS // KV_HEADS
QKV_COLS = KV_HEADS * (Q_PER_GROUP + 2) * HEAD
CAP = (2 * TOP * BATCH + EXPERTS - 1) // EXPERTS
EPS = 1e-5
ROPE_BASE = 10000.0


def gaussian(one_key, out_shape):
    return jax.random.normal(one_key, out_shape, jnp.float32)


def draw_routing(route_key):
    hot_key, shard_key = jax.random.split(route_key)
    hot_order = jax.random.permutation(hot_key, EXPERTS)
    n_pairs = TOP * BATCH
    even_total = n_pairs - n_pairs // 2
    even_rows = even_total // EXPERTS + (jnp.arange(EXPERTS) < even_total % EXPERTS).astype(jnp.int32)

    def one_shard(one_key):
        even_key, order_key = jax.random.split(one_key)
        even_order = jax.random.permutation(even_key, EXPERTS)
        counts = jnp.zeros((EXPERTS,), jnp.int32).at[even_order].set(even_rows)
        free_room = CAP - counts[hot_order]
        before = jnp.cumsum(free_room) - free_room
        extra_rows = jnp.minimum(jnp.maximum(n_pairs // 2 - before, 0), free_room)
        counts = counts.at[hot_order].add(extra_rows)
        run_ends = jnp.cumsum(counts)
        slot_expert = jnp.sum((jnp.arange(n_pairs)[:, None] >= run_ends[None, :]).astype(jnp.int32), axis=1)
        choices = slot_expert.reshape(TOP, BATCH).T
        return choices[jax.random.permutation(order_key, BATCH)]

    picked = jax.vmap(one_shard)(jax.random.split(shard_key, EP_SHARDS))
    return picked.reshape(TOKENS, TOP).astype(jnp.int32)


def draw_lengths(len_key):
    draw_key, mark_key = jax.random.split(len_key)
    lengths = jax.random.randint(draw_key, (TOKENS,), SMAX // 16, SMAX)
    mark_order = jax.random.permutation(mark_key, TOKENS)
    lengths = lengths.at[mark_order[0]].set(SMAX - 1).at[mark_order[1]].set(SMAX // 16)
    return lengths.astype(jnp.int32)


def draw_rope(rope_key, lengths, factor_min, factor_max):
    rescale = jax.random.uniform(rope_key, (HEAD // 2,), jnp.float32, factor_min, factor_max)
    inv_freq = ROPE_BASE ** (-jnp.arange(HEAD // 2, dtype=jnp.float32) * 2.0 / HEAD)
    angles = lengths.astype(jnp.float32)[:, None] * inv_freq[None, :] / rescale[None, :]
    return jnp.cos(angles), jnp.sin(angles)


def setup_inputs(seed: int = 0, part: int = 0) -> dict:
    shared_key = jax.random.key(seed)
    part_key = jax.random.fold_in(jax.random.key(seed + 1), part)
    weight_keys = jax.random.split(shared_key, 12)
    part_keys = jax.random.split(part_key, 7)
    bf16 = jnp.bfloat16
    lengths = draw_lengths(part_keys[0])
    rope_cos, rope_sin = draw_rope(part_keys[1], lengths, 1.0, 8.0)
    hidden = gaussian(part_keys[2], (TOKENS, D))
    k_cache = 2.0 * gaussian(part_keys[3], (TOKENS, SMAX, KV_HEADS, HEAD))
    v_cache = 0.5 * gaussian(part_keys[4], (TOKENS, 1, KV_HEADS, HEAD)) + gaussian(part_keys[5], (TOKENS, SMAX, KV_HEADS, HEAD))
    expert_ids = draw_routing(part_keys[6])
    return {
        'hidden': hidden.astype(bf16),
        'seq_lens': lengths,
        'rope_cos': rope_cos,
        'rope_sin': rope_sin,
        'ln1_scale': (1.0 + 0.3 * gaussian(weight_keys[0], (D,))).astype(bf16),
        'ln1_bias': (0.3 * gaussian(weight_keys[1], (D,))).astype(bf16),
        'w_qkv': (gaussian(weight_keys[2], (D, QKV_COLS)) * D ** -0.5).astype(bf16),
        'b_qkv': (0.5 * gaussian(weight_keys[3], (QKV_COLS,))).astype(bf16),
        'w_out': (gaussian(weight_keys[4], (HEADS * HEAD, D)) * (HEADS * HEAD) ** -0.5).astype(bf16),
        'b_out': (0.3 * gaussian(weight_keys[5], (D,))).astype(bf16),
        'k_cache': k_cache.astype(bf16),
        'v_cache': v_cache.astype(bf16),
        'ln2_scale': (1.0 + 0.3 * gaussian(weight_keys[6], (D,))).astype(bf16),
        'ln2_bias': (0.3 * gaussian(weight_keys[7], (D,))).astype(bf16),
        'w_router': (gaussian(weight_keys[8], (D, EXPERTS)) * D ** -0.5).astype(bf16),
        'expert_ids': expert_ids,
        'w_gate': (gaussian(weight_keys[9], (EXPERTS, D, FF)) * D ** -0.5).astype(bf16),
        'w_up': (gaussian(weight_keys[10], (EXPERTS, D, FF)) * D ** -0.5).astype(bf16),
        'w_down': (gaussian(weight_keys[11], (EXPERTS, FF, D)) * FF ** -0.5).astype(bf16),
    }


def layer_norm(values, ln_scale, ln_bias):
    vals_f32 = values.astype(jnp.float32)
    row_mean = jnp.mean(vals_f32, axis=-1, keepdims=True)
    centered = vals_f32 - row_mean
    row_var = jnp.mean(centered * centered, axis=-1, keepdims=True)
    normed = centered * lax.rsqrt(row_var + EPS)
    return (normed * ln_scale.astype(jnp.float32) + ln_bias.astype(jnp.float32)).astype(jnp.bfloat16)


def apply_rope(values, cos_part, sin_part):
    half_dim = values.shape[-1] // 2
    vals_f32 = values.astype(jnp.float32)
    first_half = vals_f32[..., :half_dim]
    second_half = vals_f32[..., half_dim:]
    rotated = jnp.concatenate([first_half * cos_part - second_half * sin_part, second_half * cos_part + first_half * sin_part], axis=-1)
    return rotated.astype(jnp.bfloat16)


def reference(hidden, seq_lens, rope_cos, rope_sin, ln1_scale, ln1_bias, w_qkv, b_qkv, w_out, b_out, k_cache, v_cache, ln2_scale, ln2_bias, w_router, expert_ids, w_gate, w_up, w_down):
    normed = layer_norm(hidden, ln1_scale, ln1_bias)
    qkv_rows = (jnp.dot(normed, w_qkv, preferred_element_type=jnp.float32) + b_qkv.astype(jnp.float32)).astype(jnp.bfloat16)
    qkv_rows = qkv_rows.reshape(TOKENS, KV_HEADS, Q_PER_GROUP + 2, HEAD)
    queries = apply_rope(qkv_rows[:, :, :Q_PER_GROUP], rope_cos[:, None, None, :], rope_sin[:, None, None, :])
    key_new = apply_rope(qkv_rows[:, :, Q_PER_GROUP], rope_cos[:, None, :], rope_sin[:, None, :])
    value_new = qkv_rows[:, :, Q_PER_GROUP + 1]
    positions = jnp.arange(SMAX)
    write_mask = (positions[None, :] == seq_lens[:, None])[:, :, None, None]
    k_cache_out = jnp.where(write_mask, key_new[:, None], k_cache)
    v_cache_out = jnp.where(write_mask, value_new[:, None], v_cache)

    def attend(per_seq):
        q_one, k_one, v_one, len_one = per_seq
        scores = jnp.einsum('gqh,sgh->gqs', q_one.astype(jnp.float32), k_one.astype(jnp.float32)) * HEAD ** -0.5
        scores = jnp.where(positions[None, None, :] <= len_one, scores, -jnp.inf)
        attn_probs = jax.nn.softmax(scores, axis=-1).astype(jnp.bfloat16)
        return jnp.einsum('gqs,sgh->gqh', attn_probs.astype(jnp.float32), v_one.astype(jnp.float32)).astype(jnp.bfloat16)

    context = lax.map(attend, (queries, k_cache_out, v_cache_out, seq_lens))
    attn_full = jnp.dot(context.reshape(TOKENS, HEADS * HEAD), w_out, preferred_element_type=jnp.float32)
    hidden_mid = (hidden.astype(jnp.float32) + attn_full + b_out.astype(jnp.float32)).astype(jnp.bfloat16)
    normed2 = layer_norm(hidden_mid, ln2_scale, ln2_bias)
    logits = jnp.dot(normed2, w_router, preferred_element_type=jnp.float32)
    chosen = jnp.take_along_axis(logits, expert_ids, axis=1)
    gate_probs = jax.nn.softmax(chosen, axis=-1).astype(jnp.bfloat16).astype(jnp.float32)
    mix_weights = jnp.sum(jax.nn.one_hot(expert_ids, EXPERTS, dtype=jnp.float32) * gate_probs[:, :, None], axis=1)

    def expert_step(moe_acc, per_expert):
        gate_w, up_w, down_w, weight = per_expert
        gate_pre = jnp.dot(normed2, gate_w, preferred_element_type=jnp.float32)
        up_pre = jnp.dot(normed2, up_w, preferred_element_type=jnp.float32)
        hidden_act = (jax.nn.silu(gate_pre) * up_pre).astype(jnp.bfloat16)
        expert_out = jnp.dot(hidden_act, down_w, preferred_element_type=jnp.float32).astype(jnp.bfloat16)
        return moe_acc + weight[:, None] * expert_out.astype(jnp.float32), None

    moe_sum, _ = lax.scan(expert_step, jnp.zeros((TOKENS, D), jnp.float32), (w_gate, w_up, w_down, mix_weights.T))
    hidden_out = (hidden_mid.astype(jnp.float32) + moe_sum).astype(jnp.bfloat16)
    return (hidden_out, k_cache_out, v_cache_out)
```

```python
import functools

import jax
import jax.numpy as jnp
from jax import lax
from jax.experimental import pallas as pl
from jax.experimental.pallas import tpu as pltpu
from jax.sharding import PartitionSpec as P

EPS = 1e-5
F32 = jnp.float32
BF16 = jnp.bfloat16
MESH = pl.DeviceIdType.MESH
NT = (((1,), (1,)), ((), ()))


def layer_norm(vals_f32, scale, bias):
    row_mean = jnp.mean(vals_f32, axis=-1, keepdims=True)
    centered = vals_f32 - row_mean
    row_var = jnp.mean(centered * centered, axis=-1, keepdims=True)
    normed = centered * lax.rsqrt(row_var + EPS)
    return (normed * scale.astype(F32) + bias.astype(F32)).astype(BF16)


def attn_kernel(seq_ref, hid_ref, cos_ref, sin_ref, lns_ref, lnb_ref, bq_ref, wq_hbm, kc_hbm, vc_hbm, wo_hbm,
                part_ref, ko_hbm, vo_hbm,
                wq_buf, kbuf, vbuf, wo_buf, hbuf, qs, ks, vs, ctx, cb,
                wq_sem, k_sem, v_sem, wo_sem, ko_sem, vo_sem):
    n_b = hid_ref.shape[0]
    n_wq, _, wq_cols = wq_buf.shape
    n_wo, _, wo_cols = wo_buf.shape
    rows = kbuf.shape[1]
    heads = qs.shape[0] // n_b
    chunk = 8
    n_chunk = n_b // chunk

    def wq_copy(n):
        return pltpu.make_async_copy(wq_hbm.at[:, pl.ds(n * wq_cols, wq_cols)], wq_buf.at[n], wq_sem.at[n])

    def k_copy(c):
        return pltpu.make_async_copy(kc_hbm.at[pl.ds(c * chunk, chunk)], kbuf.at[pl.ds(c * chunk, chunk)], k_sem.at[c])

    def v_copy(c):
        return pltpu.make_async_copy(vc_hbm.at[pl.ds(c * chunk, chunk)], vbuf.at[pl.ds(c * chunk, chunk)], v_sem.at[c])

    def wo_copy(n):
        return pltpu.make_async_copy(wo_hbm.at[:, pl.ds(n * wo_cols, wo_cols)], wo_buf.at[n], wo_sem.at[n])

    def ko_copy(c):
        return pltpu.make_async_copy(kbuf.at[pl.ds(c * chunk, chunk)], ko_hbm.at[pl.ds(c * chunk, chunk)], ko_sem.at[c])

    def vo_copy(c):
        return pltpu.make_async_copy(vbuf.at[pl.ds(c * chunk, chunk)], vo_hbm.at[pl.ds(c * chunk, chunk)], vo_sem.at[c])

    for n in range(n_wq):
        wq_copy(n).start()
    for c in range(n_chunk):
        k_copy(c).start()
        v_copy(c).start()
    for n in range(n_wo):
        wo_copy(n).start()

    hbuf[...] = layer_norm(hid_ref[...].astype(F32), lns_ref[...], lnb_ref[...])
    cos2 = jnp.concatenate([cos_ref[...], cos_ref[...]], axis=1)
    sin2 = jnp.concatenate([-sin_ref[...], sin_ref[...]], axis=1)
    per_group = heads // 2 + 2
    for n in range(n_wq):
        wq_copy(n).wait()
        cols = pl.ds(n * wq_cols, wq_cols)
        qkv = jnp.dot(hbuf[...], wq_buf[n], preferred_element_type=F32) + bq_ref[:, cols].astype(F32)
        qkv = qkv.astype(BF16).astype(F32)
        for i in range(wq_cols // 128):
            g, j = divmod(n * (wq_cols // 128) + i, per_group)
            block = qkv[:, i * 128:(i + 1) * 128]
            if j <= heads // 2:
                block = block * cos2 + pltpu.roll(block, 64, 1) * sin2
                block = block.astype(BF16).astype(F32)
            if j < heads // 2:
                qs[pl.ds(g * (heads // 2) + j, n_b, stride=heads), :] = block
            elif j == heads // 2:
                ks[pl.ds(g, n_b, stride=2), :] = block
            else:
                vs[pl.ds(g, n_b, stride=2), :] = block

    col = lax.broadcasted_iota(jnp.int32, (heads, rows), 1)
    head_row = lax.broadcasted_iota(jnp.int32, (heads, rows), 0)
    own_group = (col % 2) == (head_row // (heads // 2))
    position = jnp.where(own_group, col // 2, rows)
    tile_row = lax.broadcasted_iota(jnp.int32, (16, 128), 0)
    scale = 128 ** -0.5

    def one_chunk(c, _):
        k_copy(c).wait()
        v_copy(c).wait()
        lens = [seq_ref[c * chunk + i] for i in range(chunk)]
        for i in range(chunk):
            b = c * chunk + i
            base = pl.multiple_of((lens[i] // 8) * 16, 16)
            first = lens[i] * 2 - base
            for buf, new in ((kbuf, ks), (vbuf, vs)):
                tile = buf[b, pl.ds(base, 16), :].astype(F32)
                tile = jnp.where(tile_row == first, new[pl.ds(b * 2, 1), :], tile)
                tile = jnp.where(tile_row == first + 1, new[pl.ds(b * 2 + 1, 1), :], tile)
                buf[b, pl.ds(base, 16), :] = tile.astype(BF16)
        ko_copy(c).start()
        vo_copy(c).start()
        scores = []
        for i in range(chunk):
            b = c * chunk + i
            q = qs[pl.ds(pl.multiple_of(b * heads, heads), heads), :].astype(BF16)
            s = lax.dot_general(q, kbuf[b], NT, preferred_element_type=F32) * scale
            scores.append(jnp.where(position <= lens[i], s, -jnp.inf))
        probs = []
        for i in range(chunk):
            top = jnp.max(scores[i], axis=-1, keepdims=True)
            e = jnp.exp(scores[i] - top)
            probs.append((e / jnp.sum(e, axis=-1, keepdims=True)).astype(BF16))
        for i in range(chunk):
            b = c * chunk + i
            out = jnp.dot(probs[i], vbuf[b], preferred_element_type=F32)
            ctx[pl.ds(pl.multiple_of(b * heads, heads), heads), :] = out.astype(BF16).astype(F32)
        return 0

    lax.fori_loop(0, n_chunk, one_chunk, 0)
    for j in range(heads):
        cb[:, j * 128:(j + 1) * 128] = ctx[pl.ds(j, n_b, stride=heads), :].astype(BF16)
    for n in range(n_wo):
        wo_copy(n).wait()
        part_ref[:, pl.ds(n * wo_cols, wo_cols)] = jnp.dot(cb[...], wo_buf[n], preferred_element_type=F32).astype(BF16)
    for c in range(n_chunk):
        ko_copy(c).wait()
        vo_copy(c).wait()


def attention_call(hidden, seq_lens, rope_cos, rope_sin, ln_scale, ln_bias, w_qkv, b_qkv, w_out, k_rows, v_rows):
    n_b, d_model = hidden.shape
    heads = w_out.shape[0] // 128
    vmem = pl.BlockSpec(memory_space=pltpu.VMEM)
    hbm = pl.BlockSpec(memory_space=pl.ANY)
    wq_cols = 512
    wo_cols = 512
    n_wq = w_qkv.shape[1] // wq_cols
    n_wo = d_model // wo_cols
    dma = pltpu.SemaphoreType.DMA
    return pl.pallas_call(
        attn_kernel,
        out_shape=(
            jax.ShapeDtypeStruct((n_b, d_model), BF16),
            jax.ShapeDtypeStruct(k_rows.shape, BF16),
            jax.ShapeDtypeStruct(v_rows.shape, BF16),
        ),
        in_specs=[pl.BlockSpec(memory_space=pltpu.SMEM)] + [vmem] * 6 + [hbm] * 4,
        out_specs=(vmem, hbm, hbm),
        scratch_shapes=[
            pltpu.VMEM((n_wq, d_model, wq_cols), BF16),
            pltpu.VMEM(k_rows.shape, BF16),
            pltpu.VMEM(v_rows.shape, BF16),
            pltpu.VMEM((n_wo, w_out.shape[0], wo_cols), BF16),
            pltpu.VMEM((n_b, d_model), BF16),
            pltpu.VMEM((n_b * heads, 128), F32),
            pltpu.VMEM((n_b * 2, 128), F32),
            pltpu.VMEM((n_b * 2, 128), F32),
            pltpu.VMEM((n_b * heads, 128), F32),
            pltpu.VMEM((n_b, heads * 128), BF16),
            dma((n_wq,)), dma((n_b // 8,)), dma((n_b // 8,)), dma((n_wo,)), dma((n_b // 8,)), dma((n_b // 8,)),
        ],
        compiler_params=pltpu.CompilerParams(vmem_limit_bytes=60 * 1024 * 1024),
        name="attn",
    )(seq_lens, hidden, rope_cos, rope_sin, ln_scale, ln_bias, b_qkv, w_qkv, k_rows, v_rows, w_out)


def moe_kernel(n_tp, n_ep, part_ref, hid_ref, bout_ref, lns_ref, lnb_ref, wr_ref, ids_ref, wg_hbm, wu_hbm, wd_hbm,
               out_ref,
               gbuf, ubuf, dbuf, hall, arx, x1buf, dmat, cmat, xbuf, abuf, ybuf, pbuf, rbuf, obuf,
               gsem, usem, dsem, a_send, a_recv, h_send, h_recv, r_send, r_recv, o_send, o_recv):
    me_t = lax.axis_index("tp")
    me_e = lax.axis_index("ep")
    n_dev = n_tp * n_ep
    me = me_e * n_tp + me_t
    n_gu, d_model, width = gbuf.shape
    n_dr, d_group, _, d_cols = dbuf.shape
    n_local = wg_hbm.shape[0]
    n_exp = n_local * n_ep
    half = x1buf.shape[0]
    shard = half * n_tp
    n_rows = hall.shape[0]
    cap = 32
    n_col = d_model // d_cols
    n_grp = n_local // d_group
    n_down = n_col * n_grp

    def peer_of(d):
        pid = lax.rem(me + d, n_dev)
        return pid, {"tp": lax.rem(pid, n_tp), "ep": lax.div(pid, n_tp)}

    def g_copy(i):
        slot = lax.rem(i, n_gu)
        return pltpu.make_async_copy(wg_hbm.at[i], gbuf.at[slot], gsem.at[slot])

    def u_copy(i):
        slot = lax.rem(i, n_gu)
        return pltpu.make_async_copy(wu_hbm.at[i], ubuf.at[slot], usem.at[slot])

    def d_copy(q):
        slot = lax.rem(q, n_dr)
        grp = lax.rem(q, n_grp)
        col = lax.div(q, n_grp)
        src = wd_hbm.at[pl.ds(grp * d_group, d_group), :, pl.ds(pl.multiple_of(col * d_cols, d_cols), d_cols)]
        return pltpu.make_async_copy(src, dbuf.at[slot], dsem.at[slot])

    def first_gu(i, _):
        g_copy(i).start()
        u_copy(i).start()
        return 0

    def first_d(q, _):
        d_copy(q).start()
        return 0

    lax.fori_loop(0, n_gu, first_gu, 0)
    lax.fori_loop(0, n_dr, first_d, 0)

    barrier = pltpu.get_barrier_semaphore()
    for d in range(1, n_dev):
        _, dev = peer_of(d)
        pl.semaphore_signal(barrier, inc=1, device_id=dev, device_id_type=MESH)
    pl.semaphore_wait(barrier, n_dev - 1)

    other_t = 1 - me_t
    a_copy = pltpu.make_async_remote_copy(
        src_ref=part_ref.at[pl.ds(pl.multiple_of(other_t * half, half), half)], dst_ref=arx,
        send_sem=a_send, recv_sem=a_recv, device_id={"tp": other_t, "ep": me_e}, device_id_type=MESH)
    a_copy.start()

    picked_t = jnp.zeros((n_exp, shard), F32)
    exp_row = lax.broadcasted_iota(jnp.int32, (n_exp, shard), 0)
    for k in range(ids_ref.shape[0]):
        picked_t = picked_t + (exp_row == ids_ref[pl.ds(k, 1), :]).astype(F32)
    sel = (lax.broadcasted_iota(jnp.int32, (half, shard), 1)
           == lax.broadcasted_iota(jnp.int32, (half, shard), 0) + me_t * half).astype(BF16)
    picked = lax.dot_general(sel, picked_t.astype(BF16), NT, preferred_element_type=F32)

    mine = pl.ds(pl.multiple_of(me_t * half, half), half)
    a_copy.wait()
    attn = part_ref[mine, :].astype(F32) + arx[...].astype(F32)
    x1 = (hid_ref[mine, :].astype(F32) + attn + bout_ref[...].astype(F32)).astype(BF16)
    x1buf[...] = x1
    h2 = layer_norm(x1.astype(F32), lns_ref[...], lnb_ref[...])
    my_rows = pl.ds(pl.multiple_of(me * half, half), half)
    hall[my_rows, pl.ds(0, d_model)] = h2
    logits = jnp.dot(h2, wr_ref[...], preferred_element_type=F32)
    logits = jnp.where(picked > 0.5, logits, -jnp.inf)
    e = jnp.exp(logits - jnp.max(logits, axis=-1, keepdims=True))
    gates = e / jnp.sum(e, axis=-1, keepdims=True)
    hall[my_rows, pl.ds(d_model, n_exp)] = gates.astype(BF16)

    def h_copy(d, block, dev):
        rows = pl.ds(pl.multiple_of(block * half, half), half)
        return pltpu.make_async_remote_copy(
            src_ref=hall.at[rows], dst_ref=hall.at[rows], send_sem=h_send.at[d], recv_sem=h_recv.at[block],
            device_id=dev, device_id_type=MESH)

    for d in range(1, n_dev):
        _, dev = peer_of(d)
        h_copy(d, me, dev).start()
    for d in range(1, n_dev):
        pid, dev = peer_of(d)
        h_copy(d, pid, dev).wait_recv()

    gate_cols = pl.ds(d_model, n_exp)
    pick = (lax.broadcasted_iota(jnp.int32, (n_local, n_exp), 1)
            == lax.broadcasted_iota(jnp.int32, (n_local, n_exp), 0) + me_e * n_local).astype(BF16)
    row_i = lax.broadcasted_iota(jnp.int32, (n_rows, n_rows), 0)
    col_i = lax.broadcasted_iota(jnp.int32, (n_rows, n_rows), 1)
    same = (row_i // shard) == (col_i // shard)

    gate_t = lax.dot_general(pick, hall[:, gate_cols], NT, preferred_element_type=F32)
    upper = jnp.where((row_i < col_i) & same, 1.0, 0.0).astype(BF16)
    rank_t = jnp.dot(jnp.where(gate_t > 0, 1.0, 0.0).astype(BF16), upper, preferred_element_type=F32)
    shard_t = (lax.broadcasted_iota(jnp.int32, (n_local, n_rows), 1) // shard * (cap // n_ep)).astype(F32)
    key_t = jnp.where(gate_t > 0, rank_t + shard_t, -1.0)
    slot_i = lax.broadcasted_iota(jnp.int32, (cap, n_rows), 0).astype(F32)
    for i in range(n_local):
        dmat[i * cap:(i + 1) * cap, :] = jnp.where(key_t[i:i + 1, :] == slot_i, 1.0, 0.0).astype(BF16)

    def expert_group(g, _):
        rows = pl.ds(pl.multiple_of(g * d_group * cap, d_group * cap), d_group * cap)
        for c in range(4):
            cols = pl.ds(c * (d_model // 4), d_model // 4)
            xbuf[:, cols] = jnp.dot(dmat[rows, :], hall[:, cols], preferred_element_type=F32).astype(BF16)

        def one_expert(k, _):
            i = g * d_group + k
            slot = lax.rem(i, n_gu)
            x = xbuf[pl.ds(pl.multiple_of(k * cap, cap), cap), :]
            g_copy(i).wait()
            u_copy(i).wait()
            gate_pre = jnp.dot(x, gbuf[slot], preferred_element_type=F32)
            up_pre = jnp.dot(x, ubuf[slot], preferred_element_type=F32)
            act = (gate_pre * jax.nn.sigmoid(gate_pre) * up_pre).astype(BF16)
            abuf[pl.ds(pl.multiple_of(i * cap, cap), cap), :] = act

            @pl.when(i + n_gu < n_local)
            def _():
                g_copy(i + n_gu).start()
                u_copy(i + n_gu).start()

            return 0

        lax.fori_loop(0, d_group, one_expert, 0)
        return 0

    lax.fori_loop(0, n_grp - 1, expert_group, 0)

    gate_l = lax.dot_general(hall[:, gate_cols], pick, NT, preferred_element_type=F32)
    lower = jnp.where((row_i > col_i) & same, 1.0, 0.0).astype(BF16)
    rank_l = jnp.dot(lower, jnp.where(gate_l > 0, 1.0, 0.0).astype(BF16), preferred_element_type=F32)
    shard_l = (lax.broadcasted_iota(jnp.int32, (n_rows, n_local), 0) // shard * (cap // n_ep)).astype(F32)
    key_l = jnp.where(gate_l > 0, rank_l + shard_l, -1.0).astype(BF16)
    gate_b = gate_l.astype(BF16)
    step = 256
    for c in range(n_local * cap // step):
        spread = (lax.broadcasted_iota(jnp.int32, (n_local, step), 0)
                  == (lax.broadcasted_iota(jnp.int32, (n_local, step), 1) + c * step) // cap).astype(BF16)
        key_x = jnp.dot(key_l, spread, preferred_element_type=F32)
        gate_x = jnp.dot(gate_b, spread, preferred_element_type=F32)
        lane = (lax.broadcasted_iota(jnp.int32, (n_rows, step), 1) % cap).astype(F32)
        cmat[:, pl.ds(c * step, step)] = jnp.where(key_x == lane, gate_x, 0.0).astype(BF16)

    lax.fori_loop(n_grp - 1, n_grp, expert_group, 0)

    def r_copy(j, d, block_sent, block_from, dev):
        rows = pl.ds(pl.multiple_of(block_sent * half, half), half)
        return pltpu.make_async_remote_copy(
            src_ref=pbuf.at[j, rows], dst_ref=rbuf.at[j, block_from], send_sem=r_send.at[j, d],
            recv_sem=r_recv.at[j, block_from], device_id=dev, device_id_type=MESH)

    def o_copy(j, block_t):
        return pltpu.make_async_remote_copy(
            src_ref=obuf.at[j, block_t], dst_ref=obuf.at[j, block_t], send_sem=o_send.at[j], recv_sem=o_recv.at[j],
            device_id={"tp": other_t, "ep": me_e}, device_id_type=MESH)

    def finish(j):
        cols = pl.ds(pl.multiple_of(j * d_cols, d_cols), d_cols)
        total = pbuf[j, my_rows, :].astype(F32)
        for d in range(1, n_dev):
            pid, dev = peer_of(d)
            r_copy(j, d, pid, pid, dev).wait_recv()
            total = total + rbuf[j, pid].astype(F32)
        obuf[j, me_t] = (x1buf[:, cols].astype(F32) + total).astype(BF16)
        o_copy(j, me_t).start()

    lag = 2

    def one_col(j, _):
        def one_part(g, _):
            q = j * n_grp + g
            slot = lax.rem(q, n_dr)
            d_copy(q).wait()
            for k in range(d_group):
                rows = pl.ds(pl.multiple_of((g * d_group + k) * cap, cap), cap)
                ybuf[rows, :] = jnp.dot(abuf[rows, :], dbuf[slot, k], preferred_element_type=F32).astype(BF16)

            @pl.when(q + n_dr < n_down)
            def _():
                d_copy(q + n_dr).start()

            return 0

        lax.fori_loop(0, n_grp, one_part, 0)
        pbuf[j] = jnp.dot(cmat[...], ybuf[...], preferred_element_type=F32).astype(BF16)
        for d in range(1, n_dev):
            pid, dev = peer_of(d)
            r_copy(j, d, pid, me, dev).start()

        @pl.when(j >= lag)
        def _():
            finish(j - lag)

        return 0

    lax.fori_loop(0, n_col, one_col, 0)
    for j in range(n_col - lag, n_col):
        finish(j)

    def drain(j, _):
        for d in range(1, n_dev):
            pid, dev = peer_of(d)
            r_copy(j, d, pid, me, dev).wait_send()
        o_copy(j, me_t).wait_send()
        return 0

    lax.fori_loop(0, n_col, drain, 0)
    for d in range(1, n_dev):
        _, dev = peer_of(d)
        h_copy(d, me, dev).wait_send()
    for j in range(n_col):
        o_copy(j, other_t).wait_recv()
        for t in range(n_tp):
            out_ref[t * half:(t + 1) * half, j * d_cols:(j + 1) * d_cols] = obuf[j, t]


def moe_call(n_tp, n_ep, part, hidden, b_out, ln_scale, ln_bias, w_router, ids_t, w_gate, w_up, w_down):
    n_b, d_model = hidden.shape
    n_local, _, width = w_gate.shape
    n_exp = n_local * n_ep
    n_rows = n_b * n_ep
    n_dev = n_tp * n_ep
    half = n_b // n_tp
    cap = 32
    n_gu, n_dr, d_group, d_cols = 9, 12, 8, 256
    n_col = d_model // d_cols
    vmem = pl.BlockSpec(memory_space=pltpu.VMEM)
    hbm = pl.BlockSpec(memory_space=pl.ANY)
    dma = pltpu.SemaphoreType.DMA
    return pl.pallas_call(
        functools.partial(moe_kernel, n_tp, n_ep),
        out_shape=jax.ShapeDtypeStruct((n_b, d_model), BF16),
        in_specs=[vmem] * 7 + [hbm] * 3,
        out_specs=vmem,
        scratch_shapes=[
            pltpu.VMEM((n_gu, d_model, width), BF16),
            pltpu.VMEM((n_gu, d_model, width), BF16),
            pltpu.VMEM((n_dr, d_group, width, d_cols), BF16),
            pltpu.VMEM((n_rows, d_model + n_exp), BF16),
            pltpu.VMEM((half, d_model), BF16),
            pltpu.VMEM((half, d_model), BF16),
            pltpu.VMEM((n_local * cap, n_rows), BF16),
            pltpu.VMEM((n_rows, n_local * cap), BF16),
            pltpu.VMEM((d_group * cap, d_model), BF16),
            pltpu.VMEM((n_local * cap, width), BF16),
            pltpu.VMEM((n_local * cap, d_cols), BF16),
            pltpu.VMEM((n_col, n_rows, d_cols), BF16),
            pltpu.VMEM((n_col, n_dev, half, d_cols), BF16),
            pltpu.VMEM((n_col, n_tp, half, d_cols), BF16),
            dma((n_gu,)), dma((n_gu,)), dma((n_dr,)), dma, dma, dma((n_dev,)), dma((n_dev,)),
            dma((n_col, n_dev)), dma((n_col, n_dev)), dma((n_col,)), dma((n_col,)),
        ],
        compiler_params=pltpu.CompilerParams(
            collective_id=0, has_side_effects=True, vmem_limit_bytes=67043328),
        name="moe",
    )(part, hidden, b_out, ln_scale, ln_bias, w_router, ids_t, w_gate, w_up, w_down)


def solution(mesh):
    n_tp, n_ep = mesh.shape['tp'], mesh.shape['ep']
    token_rows = P(('dp', 'ep'), None)
    token_vec = P(('dp', 'ep'))
    cache_spec = P(('dp', 'ep'), None, 'tp', None)
    expert_in = P('ep', None, 'tp')
    expert_down = P('ep', 'tp', None)

    def device_step(hidden, seq_lens, rope_cos, rope_sin, ln1_scale, ln1_bias, w_qkv, b_qkv, w_out, b_out, k_cache, v_cache, ln2_scale, ln2_bias, w_router, expert_ids, w_gate, w_up, w_down):
        n_b, s_max, n_groups, head = k_cache.shape
        k_rows = k_cache.reshape(n_b, s_max * n_groups, head)
        v_rows = v_cache.reshape(n_b, s_max * n_groups, head)
        part, k_out, v_out = attention_call(
            hidden, seq_lens, rope_cos, rope_sin, ln1_scale[None], ln1_bias[None], w_qkv, b_qkv[None], w_out, k_rows, v_rows)
        hidden_out = moe_call(
            n_tp, n_ep, part, hidden, b_out[None], ln2_scale[None], ln2_bias[None], w_router, expert_ids.T, w_gate, w_up, w_down)
        return hidden_out, k_out.reshape(k_cache.shape), v_out.reshape(v_cache.shape)

    in_specs = (token_rows, token_vec, token_rows, token_rows, P(), P(), P(None, 'tp'), P('tp'), P('tp', None), P(), cache_spec, cache_spec, P(), P(), P(), token_rows, expert_in, expert_in, expert_down)
    return jax.shard_map(device_step, mesh=mesh, in_specs=in_specs, out_specs=(token_rows, cache_spec, cache_spec), check_vma=False)
```

```python
import functools

import jax
import jax.numpy as jnp
from jax import lax
from jax.experimental import pallas as pl
from jax.experimental.pallas import tpu as pltpu
from jax.sharding import PartitionSpec as P

EPS = 1e-5
F32 = jnp.float32
BF16 = jnp.bfloat16
MESH = pl.DeviceIdType.MESH
NT = (((1,), (1,)), ((), ()))


def as_row(vec):
    return vec.astype(F32).reshape(1, vec.shape[0])


def layer_norm(vals_f32, scale, bias):
    row_mean = jnp.mean(vals_f32, axis=-1, keepdims=True)
    centered = vals_f32 - row_mean
    row_var = jnp.mean(centered * centered, axis=-1, keepdims=True)
    normed = centered * lax.rsqrt(row_var + EPS)
    return (normed * as_row(scale) + as_row(bias)).astype(BF16)


def load_all(sources, targets, sems):
    copies = [pltpu.make_async_copy(src, dst, sems.at[i]) for i, (src, dst) in enumerate(zip(sources, targets))]
    for copy in copies:
        copy.start()
    return copies


def attn_kernel(seq_ref, hid_ref, cos_ref, sin_ref, lns_ref, lnb_ref, bq_ref, wq_hbm, kc_hbm, vc_hbm, wo_hbm,
                part_ref, ko_hbm, vo_hbm,
                wq_buf, kbuf, vbuf, wo_buf, hbuf, qs, ks, vs, ctx, cb,
                wq_sem, k_sem, v_sem, wo_sem, ko_sem, vo_sem):
    n_b = hid_ref.shape[0]
    n_wq, _, wq_cols = wq_buf.shape
    n_wo, _, wo_cols = wo_buf.shape
    rows = kbuf.shape[1]
    heads = qs.shape[0] // n_b
    chunk = 16
    n_chunk = n_b // chunk

    def wq_copy(n):
        return pltpu.make_async_copy(wq_hbm.at[:, pl.ds(n * wq_cols, wq_cols)], wq_buf.at[n], wq_sem.at[n])

    def k_copy(c):
        return pltpu.make_async_copy(kc_hbm.at[pl.ds(c * chunk, chunk)], kbuf.at[pl.ds(c * chunk, chunk)], k_sem.at[c])

    def v_copy(c):
        return pltpu.make_async_copy(vc_hbm.at[pl.ds(c * chunk, chunk)], vbuf.at[pl.ds(c * chunk, chunk)], v_sem.at[c])

    def wo_copy(n):
        return pltpu.make_async_copy(wo_hbm.at[:, pl.ds(n * wo_cols, wo_cols)], wo_buf.at[n], wo_sem.at[n])

    def ko_copy(c):
        return pltpu.make_async_copy(kbuf.at[pl.ds(c * chunk, chunk)], ko_hbm.at[pl.ds(c * chunk, chunk)], ko_sem.at[c])

    def vo_copy(c):
        return pltpu.make_async_copy(vbuf.at[pl.ds(c * chunk, chunk)], vo_hbm.at[pl.ds(c * chunk, chunk)], vo_sem.at[c])

    stages = [[] for _ in range(n_wq)]
    first = [wq_copy(n) for n in range(n_wq)] + [k_copy(0), v_copy(0)]
    for c in range(1, n_chunk):
        stages[min(c - 1, n_wq - 1)] += [k_copy(c), v_copy(c)]
    for n in range(n_wo):
        stages[min(n_chunk - 1 + n // 2, n_wq - 1)].append(wo_copy(n))
    for copy in first:
        copy.start()

    hbuf[...] = layer_norm(hid_ref[...].astype(F32), lns_ref[...], lnb_ref[...])
    cos2 = jnp.concatenate([cos_ref[...], cos_ref[...]], axis=1)
    sin2 = jnp.concatenate([-sin_ref[...], sin_ref[...]], axis=1)
    per_group = heads // 2 + 2
    for n in range(n_wq):
        wq_copy(n).wait()
        for copy in stages[n]:
            copy.start()
        cols = pl.ds(n * wq_cols, wq_cols)
        qkv = jnp.dot(hbuf[...], wq_buf[n], preferred_element_type=F32) + as_row(bq_ref[cols])
        qkv = qkv.astype(BF16).astype(F32)
        for i in range(wq_cols // 128):
            g, j = divmod(n * (wq_cols // 128) + i, per_group)
            block = qkv[:, i * 128:(i + 1) * 128]
            if j <= heads // 2:
                block = block * cos2 + pltpu.roll(block, 64, 1) * sin2
                block = block.astype(BF16).astype(F32)
            if j < heads // 2:
                qs[pl.ds(g * (heads // 2) + j, n_b, stride=heads), :] = block
            elif j == heads // 2:
                ks[pl.ds(g, n_b, stride=2), :] = block
            else:
                vs[pl.ds(g, n_b, stride=2), :] = block

    col = lax.broadcasted_iota(jnp.int32, (heads, rows), 1)
    head_row = lax.broadcasted_iota(jnp.int32, (heads, rows), 0)
    own_group = (col % 2) == (head_row // (heads // 2))
    position = jnp.where(own_group, col // 2, rows)
    tile_row = lax.broadcasted_iota(jnp.int32, (16, 128), 0)
    scale = 128 ** -0.5

    def one_chunk(c, _):
        k_copy(c).wait()
        v_copy(c).wait()
        lens = [seq_ref[c * chunk + i] for i in range(chunk)]
        for i in range(chunk):
            b = c * chunk + i
            base = pl.multiple_of((lens[i] // 8) * 16, 16)
            first = lens[i] * 2 - base
            for buf, new in ((kbuf, ks), (vbuf, vs)):
                tile = buf[b, pl.ds(base, 16), :].astype(F32)
                tile = jnp.where(tile_row == first, new[pl.ds(b * 2, 1), :], tile)
                tile = jnp.where(tile_row == first + 1, new[pl.ds(b * 2 + 1, 1), :], tile)
                buf[b, pl.ds(base, 16), :] = tile.astype(BF16)
        ko_copy(c).start()
        vo_copy(c).start()
        scores = []
        for i in range(chunk):
            b = c * chunk + i
            q = qs[pl.ds(pl.multiple_of(b * heads, heads), heads), :].astype(BF16)
            s = lax.dot_general(q, kbuf[b], NT, preferred_element_type=F32) * scale
            scores.append(jnp.where(position <= lens[i], s, -jnp.inf))
        probs = []
        for i in range(chunk):
            top = jnp.max(scores[i], axis=-1, keepdims=True)
            e = jnp.exp(scores[i] - top)
            probs.append((e / jnp.sum(e, axis=-1, keepdims=True)).astype(BF16))
        for i in range(chunk):
            b = c * chunk + i
            out = jnp.dot(probs[i], vbuf[b], preferred_element_type=F32)
            ctx[pl.ds(pl.multiple_of(b * heads, heads), heads), :] = out.astype(BF16).astype(F32)
        return 0

    lax.fori_loop(0, n_chunk, one_chunk, 0)
    for j in range(heads):
        cb[:, j * 128:(j + 1) * 128] = ctx[pl.ds(j, n_b, stride=heads), :].astype(BF16)
    for n in range(n_wo):
        wo_copy(n).wait()
        part_ref[:, pl.ds(n * wo_cols, wo_cols)] = jnp.dot(cb[...], wo_buf[n], preferred_element_type=F32).astype(BF16)
    for c in range(n_chunk):
        ko_copy(c).wait()
        vo_copy(c).wait()


def attention_call(hidden, seq_lens, rope_cos, rope_sin, ln_scale, ln_bias, w_qkv, b_qkv, w_out, k_rows, v_rows):
    n_b, d_model = hidden.shape
    heads = w_out.shape[0] // 128
    vmem = pl.BlockSpec(memory_space=pltpu.VMEM)
    hbm = pl.BlockSpec(memory_space=pl.ANY)
    wq_cols = 512
    wo_cols = 512
    n_wq = w_qkv.shape[1] // wq_cols
    n_wo = d_model // wo_cols
    dma = pltpu.SemaphoreType.DMA
    return pl.pallas_call(
        attn_kernel,
        out_shape=(
            jax.ShapeDtypeStruct((n_b, d_model), BF16),
            jax.ShapeDtypeStruct(k_rows.shape, BF16),
            jax.ShapeDtypeStruct(v_rows.shape, BF16),
        ),
        in_specs=[pl.BlockSpec(memory_space=pltpu.SMEM)] + [vmem] * 6 + [hbm] * 4,
        out_specs=(vmem, hbm, hbm),
        scratch_shapes=[
            pltpu.VMEM((n_wq, d_model, wq_cols), BF16),
            pltpu.VMEM(k_rows.shape, BF16),
            pltpu.VMEM(v_rows.shape, BF16),
            pltpu.VMEM((n_wo, w_out.shape[0], wo_cols), BF16),
            pltpu.VMEM((n_b, d_model), BF16),
            pltpu.VMEM((n_b * heads, 128), F32),
            pltpu.VMEM((n_b * 2, 128), F32),
            pltpu.VMEM((n_b * 2, 128), F32),
            pltpu.VMEM((n_b * heads, 128), F32),
            pltpu.VMEM((n_b, heads * 128), BF16),
            dma((n_wq,)), dma((n_b // 16,)), dma((n_b // 16,)), dma((n_wo,)), dma((n_b // 16,)), dma((n_b // 16,)),
        ],
        compiler_params=pltpu.CompilerParams(vmem_limit_bytes=60 * 1024 * 1024),
        name="attn",
    )(seq_lens, hidden, rope_cos, rope_sin, ln_scale, ln_bias, b_qkv, w_qkv, k_rows, v_rows, w_out)


def moe_kernel(n_tp, n_ep, part_in, hid_in, bout_in, lns_in, lnb_in, wr_in, ids_in, wg_hbm, wu_hbm, wd_hbm,
               out_ref,
               part_ref, hid_ref, bout_ref, lns_ref, lnb_ref, wr_ref, ids_ref, in_sem,
               gubuf, dbuf, hall, arx, x1buf, dmat, cmat, xbuf, abuf, ybuf, pbuf, rbuf, obuf,
               gsem, usem, dsem, a_send, a_recv, h_send, h_recv, r_send, r_recv, o_send, o_recv):
    me_t = lax.axis_index("tp")
    me_e = lax.axis_index("ep")
    n_dev = n_tp * n_ep
    me = me_e * n_tp + me_t
    n_gu, d_model, _ = gubuf.shape
    width = wg_hbm.shape[2]
    n_dr, d_group, _, d_cols = dbuf.shape
    n_local = wg_hbm.shape[0]
    n_exp = n_local * n_ep
    half = x1buf.shape[0]
    shard = half * n_tp
    n_rows = hall.shape[0]
    cap = 32
    n_col = d_model // d_cols
    n_grp = n_local // d_group
    n_down = n_col * n_grp
    x_group = xbuf.shape[0] // cap
    n_xg = n_local // x_group
    n_unroll = 2

    def peer_of(d):
        pid = lax.rem(me + d, n_dev)
        return pid, {"tp": lax.rem(pid, n_tp), "ep": lax.div(pid, n_tp)}

    def g_copy(i):
        slot = lax.rem(i, n_gu)
        return pltpu.make_async_copy(wg_hbm.at[i], gubuf.at[slot, :, pl.ds(0, width)], gsem.at[slot])

    def u_copy(i):
        slot = lax.rem(i, n_gu)
        return pltpu.make_async_copy(wu_hbm.at[i], gubuf.at[slot, :, pl.ds(width, width)], usem.at[slot])

    def d_copy(q):
        slot = lax.rem(q, n_dr)
        grp = lax.rem(q, n_grp)
        col = lax.div(q, n_grp)
        src = wd_hbm.at[pl.ds(grp * d_group, d_group), :, pl.ds(pl.multiple_of(col * d_cols, d_cols), d_cols)]
        return pltpu.make_async_copy(src, dbuf.at[slot], dsem.at[slot])

    def first_gu(i, _):
        g_copy(i).start()
        u_copy(i).start()
        return 0

    def first_d(q, _):
        d_copy(q).start()
        return 0

    barrier = pltpu.get_barrier_semaphore()
    for d in range(1, n_dev):
        _, dev = peer_of(d)
        pl.semaphore_signal(barrier, inc=1, device_id=dev, device_id_type=MESH)
    small = load_all((part_in, hid_in, bout_in, lns_in, lnb_in, wr_in, ids_in),
                     (part_ref, hid_ref, bout_ref, lns_ref, lnb_ref, wr_ref, ids_ref), in_sem)
    lax.fori_loop(0, n_gu, first_gu, 0)
    lax.fori_loop(0, n_dr, first_d, 0)
    for copy in small:
        copy.wait()
    pl.semaphore_wait(barrier, n_dev - 1)

    other_t = 1 - me_t
    core = lax.rem(me_e, 2)
    sib_e = me_e + 1 - 2 * core
    far_e = lax.rem(me_e + 2, n_ep)
    near_dev = {"tp": me_t, "ep": sib_e}
    n_sub = a_send.shape[0]
    sub = half // n_sub

    def a_copy(s):
        rows = pl.ds(pl.multiple_of(other_t * half + s * sub, sub), sub)
        return pltpu.make_async_remote_copy(
            src_ref=part_ref.at[rows], dst_ref=arx.at[pl.ds(s * sub, sub)], send_sem=a_send.at[s],
            recv_sem=a_recv.at[s], device_id={"tp": other_t, "ep": me_e}, device_id_type=MESH)

    for s in range(n_sub):
        a_copy(s).start()

    def h_copy(step, s, block_e, block_t, dev):
        block = block_e * n_tp + block_t
        rows = pl.ds(pl.multiple_of(block * half + s * sub, sub), sub)
        return pltpu.make_async_remote_copy(
            src_ref=hall.at[rows], dst_ref=hall.at[rows], send_sem=h_send.at[step, s], recv_sem=h_recv.at[block, s],
            device_id=dev, device_id_type=MESH)

    far_dev = {"tp": me_t, "ep": far_e}
    side_dev = {"tp": other_t, "ep": me_e}
    diag_dev = {"tp": other_t, "ep": far_e}
    sends = (
        (0, me_e, me_t, far_dev), (1, me_e, me_t, side_dev), (2, me_e, me_t, near_dev), (3, me_e, me_t, diag_dev),
        (4, far_e, me_t, near_dev), (5, me_e, other_t, near_dev), (6, far_e, other_t, near_dev))

    picked_t = jnp.zeros((n_exp, shard), F32)
    exp_row = lax.broadcasted_iota(jnp.int32, (n_exp, shard), 0)
    for k in range(ids_ref.shape[0]):
        picked_t = picked_t + (exp_row == ids_ref[pl.ds(k, 1), :]).astype(F32)
    sel = (lax.broadcasted_iota(jnp.int32, (half, shard), 1)
           == lax.broadcasted_iota(jnp.int32, (half, shard), 0) + me_t * half).astype(BF16)
    picked = lax.dot_general(sel, picked_t.astype(BF16), NT, preferred_element_type=F32)

    my_rows = pl.ds(pl.multiple_of(me * half, half), half)
    for s in range(n_sub):
        rows = pl.ds(pl.multiple_of(me_t * half + s * sub, sub), sub)
        attn = part_ref[rows, :].astype(F32)
        base = hid_ref[rows, :].astype(F32)
        a_copy(s).wait_recv()
        attn = attn + arx[s * sub:(s + 1) * sub, :].astype(F32)
        x1 = (base + attn + as_row(bout_ref[...])).astype(BF16)
        x1buf[s * sub:(s + 1) * sub, :] = x1
        h2 = layer_norm(x1.astype(F32), lns_ref[...], lnb_ref[...])
        hall_rows = pl.ds(pl.multiple_of(me * half + s * sub, sub), sub)
        hall[hall_rows, pl.ds(0, d_model)] = h2
        logits = jnp.dot(h2, wr_ref[...], preferred_element_type=F32)
        logits = jnp.where(picked[s * sub:(s + 1) * sub, :] > 0.5, logits, -jnp.inf)
        e = jnp.exp(logits - jnp.max(logits, axis=-1, keepdims=True))
        gates = e / jnp.sum(e, axis=-1, keepdims=True)
        hall[hall_rows, pl.ds(d_model, n_exp)] = gates.astype(BF16)
        for step, block_e, block_t, dev in sends[:4]:
            h_copy(step, s, block_e, block_t, dev).start()

    for s in range(n_sub):
        for step, block_e, block_t, dev in sends[4:]:
            h_copy(0, s, block_e, block_t, near_dev).wait_recv()
            h_copy(step, s, block_e, block_t, dev).start()
    for s in range(n_sub):
        for block_e, block_t in ((sib_e, me_t), (sib_e, other_t), (lax.rem(sib_e + 2, n_ep), me_t),
                                 (lax.rem(sib_e + 2, n_ep), other_t)):
            h_copy(0, s, block_e, block_t, near_dev).wait_recv()

    gate_cols = pl.ds(d_model, n_exp)
    pick = (lax.broadcasted_iota(jnp.int32, (n_local, n_exp), 1)
            == lax.broadcasted_iota(jnp.int32, (n_local, n_exp), 0) + me_e * n_local).astype(BF16)
    row_i = lax.broadcasted_iota(jnp.int32, (n_rows, n_rows), 0)
    col_i = lax.broadcasted_iota(jnp.int32, (n_rows, n_rows), 1)
    same = (row_i // shard) == (col_i // shard)

    gate_t = lax.dot_general(pick, hall[:, gate_cols], NT, preferred_element_type=F32)
    upper = jnp.where((row_i < col_i) & same, 1.0, 0.0).astype(BF16)
    rank_t = jnp.dot(jnp.where(gate_t > 0, 1.0, 0.0).astype(BF16), upper, preferred_element_type=F32)
    shard_t = (lax.broadcasted_iota(jnp.int32, (n_local, n_rows), 1) // shard * (cap // n_ep)).astype(F32)
    key_t = jnp.where(gate_t > 0, rank_t + shard_t, -1.0)
    slot_i = lax.broadcasted_iota(jnp.int32, (cap, n_rows), 0).astype(F32)
    for i in range(n_local):
        dmat[i * cap:(i + 1) * cap, :] = jnp.where(key_t[i:i + 1, :] == slot_i, 1.0, 0.0).astype(BF16)

    def expert_group(g, _):
        rows = pl.ds(pl.multiple_of(g * x_group * cap, x_group * cap), x_group * cap)
        for c in range(4):
            cols = pl.ds(c * (d_model // 4), d_model // 4)
            xbuf[:, cols] = jnp.dot(dmat[rows, :], hall[:, cols], preferred_element_type=F32).astype(BF16)

        def some_experts(k, _):
            first = g * x_group + k * n_unroll
            for u in range(n_unroll):
                g_copy(first + u).wait()
                u_copy(first + u).wait()
            both = []
            for u in range(n_unroll):
                x = xbuf[pl.ds(pl.multiple_of((k * n_unroll + u) * cap, cap), cap), :]
                both.append(jnp.dot(x, gubuf[lax.rem(first + u, n_gu)], preferred_element_type=F32))
            for u in range(n_unroll):
                gate_pre, up_pre = both[u][:, :width], both[u][:, width:]
                act = (gate_pre * jax.nn.sigmoid(gate_pre) * up_pre).astype(BF16)
                abuf[pl.ds(pl.multiple_of((first + u) * cap, cap), cap), :] = act
            for u in range(n_unroll):
                i = first + u

                @pl.when(i + n_gu < n_local)
                def _():
                    g_copy(i + n_gu).start()
                    u_copy(i + n_gu).start()

            return 0

        lax.fori_loop(0, x_group // n_unroll, some_experts, 0)
        return 0

    lax.fori_loop(0, n_xg - 1, expert_group, 0)

    gate_l = lax.dot_general(hall[:, gate_cols], pick, NT, preferred_element_type=F32)
    lower = jnp.where((row_i > col_i) & same, 1.0, 0.0).astype(BF16)
    rank_l = jnp.dot(lower, jnp.where(gate_l > 0, 1.0, 0.0).astype(BF16), preferred_element_type=F32)
    shard_l = (lax.broadcasted_iota(jnp.int32, (n_rows, n_local), 0) // shard * (cap // n_ep)).astype(F32)
    key_l = jnp.where(gate_l > 0, rank_l + shard_l, -1.0).astype(BF16)
    gate_b = gate_l.astype(BF16)
    step = 256
    for c in range(n_local * cap // step):
        spread = (lax.broadcasted_iota(jnp.int32, (n_local, step), 0)
                  == (lax.broadcasted_iota(jnp.int32, (n_local, step), 1) + c * step) // cap).astype(BF16)
        key_x = jnp.dot(key_l, spread, preferred_element_type=F32)
        gate_x = jnp.dot(gate_b, spread, preferred_element_type=F32)
        lane = (lax.broadcasted_iota(jnp.int32, (n_rows, step), 1) % cap).astype(F32)
        cmat[:, pl.ds(c * step, step)] = jnp.where(key_x == lane, gate_x, 0.0).astype(BF16)

    lax.fori_loop(n_xg - 1, n_xg, expert_group, 0)

    def r_copy(j, d, block_sent, block_from, dev):
        rows = pl.ds(pl.multiple_of(block_sent * half, half), half)
        return pltpu.make_async_remote_copy(
            src_ref=pbuf.at[j, rows], dst_ref=rbuf.at[j, block_from], send_sem=r_send.at[j, d],
            recv_sem=r_recv.at[j, block_from], device_id=dev, device_id_type=MESH)

    def o_copy(j, block_t):
        return pltpu.make_async_remote_copy(
            src_ref=obuf.at[j, block_t], dst_ref=obuf.at[j, block_t], send_sem=o_send.at[j], recv_sem=o_recv.at[j],
            device_id={"tp": other_t, "ep": me_e}, device_id_type=MESH)

    def finish(j):
        cols = pl.ds(pl.multiple_of(j * d_cols, d_cols), d_cols)
        total = pbuf[j, my_rows, :].astype(F32)
        for d in range(1, n_dev):
            pid, dev = peer_of(d)
            r_copy(j, d, pid, pid, dev).wait_recv()
            total = total + rbuf[j, pid].astype(F32)
        obuf[j, me_t] = (x1buf[:, cols].astype(F32) + total).astype(BF16)
        o_copy(j, me_t).start()

    lag = 2

    def one_col(j, _):
        def one_part(g, _):
            q = j * n_grp + g
            slot = lax.rem(q, n_dr)
            d_copy(q).wait()
            main = width // 256 * 256
            rest = width - main
            pad = jnp.zeros((cap, rest), BF16)
            for k in range(0, d_group, 2):
                rows = [pl.ds(pl.multiple_of((g * d_group + k + u) * cap, cap), cap) for u in range(2)]
                acts = [abuf[rows[u], :] for u in range(2)]
                ends = jnp.concatenate([
                    jnp.concatenate([acts[0][:, main:], pad], axis=1),
                    jnp.concatenate([pad, acts[1][:, main:]], axis=1)], axis=0)
                end_w = jnp.concatenate([dbuf[slot, k, main:, :], dbuf[slot, k + 1, main:, :]], axis=0)
                tail = jnp.dot(ends, end_w, preferred_element_type=F32)
                for u in range(2):
                    y = jnp.dot(acts[u][:, :main], dbuf[slot, k + u, :main, :], preferred_element_type=F32)
                    ybuf[rows[u], :] = (y + tail[u * cap:(u + 1) * cap]).astype(BF16)

            @pl.when(q + n_dr < n_down)
            def _():
                d_copy(q + n_dr).start()

            return 0

        lax.fori_loop(0, n_grp, one_part, 0)
        for u in range(2):
            part_rows = slice(u * n_rows // 2, (u + 1) * n_rows // 2)
            pbuf[j, part_rows, :] = jnp.dot(cmat[part_rows, :], ybuf[...], preferred_element_type=F32).astype(BF16)
        for d in range(1, n_dev):
            pid, dev = peer_of(d)
            r_copy(j, d, pid, me, dev).start()

        @pl.when(j >= lag)
        def _():
            finish(j - lag)

        return 0

    lax.fori_loop(0, n_col, one_col, 0)
    for j in range(n_col - lag, n_col):
        finish(j)

    def drain(j, _):
        for d in range(1, n_dev):
            pid, dev = peer_of(d)
            r_copy(j, d, pid, me, dev).wait_send()
        o_copy(j, me_t).wait_send()
        return 0

    lax.fori_loop(0, n_col, drain, 0)
    for s in range(n_sub):
        a_copy(s).wait_send()
        for step, block_e, block_t, dev in sends:
            h_copy(step, s, block_e, block_t, dev).wait_send()
    for j in range(n_col):
        o_copy(j, other_t).wait_recv()
        for t in range(n_tp):
            out_ref[t * half:(t + 1) * half, j * d_cols:(j + 1) * d_cols] = obuf[j, t]


def moe_call(n_tp, n_ep, part, hidden, b_out, ln_scale, ln_bias, w_router, ids_t, w_gate, w_up, w_down):
    n_b, d_model = hidden.shape
    n_local, _, width = w_gate.shape
    n_exp = n_local * n_ep
    n_rows = n_b * n_ep
    n_dev = n_tp * n_ep
    half = n_b // n_tp
    cap = 32
    n_gu, n_dr, d_group, d_cols = 12, 4, 16, 256
    n_sub = 2
    n_col = d_model // d_cols
    vmem = pl.BlockSpec(memory_space=pltpu.VMEM)
    hbm = pl.BlockSpec(memory_space=pl.ANY)
    dma = pltpu.SemaphoreType.DMA
    return pl.pallas_call(
        functools.partial(moe_kernel, n_tp, n_ep),
        out_shape=jax.ShapeDtypeStruct((n_b, d_model), BF16),
        in_specs=[hbm] * 10,
        out_specs=vmem,
        scratch_shapes=[pltpu.VMEM(x.shape, x.dtype) for x in (part, hidden, b_out, ln_scale, ln_bias, w_router, ids_t)] + [
            dma((7,)),
            pltpu.VMEM((n_gu, d_model, 2 * width), BF16),
            pltpu.VMEM((n_dr, d_group, width, d_cols), BF16),
            pltpu.VMEM((n_rows, d_model + n_exp), BF16),
            pltpu.VMEM((half, d_model), BF16),
            pltpu.VMEM((half, d_model), BF16),
            pltpu.VMEM((n_local * cap, n_rows), BF16),
            pltpu.VMEM((n_rows, n_local * cap), BF16),
            pltpu.VMEM((8 * cap, d_model), BF16),
            pltpu.VMEM((n_local * cap, width), BF16),
            pltpu.VMEM((n_local * cap, d_cols), BF16),
            pltpu.VMEM((n_col, n_rows, d_cols), BF16),
            pltpu.VMEM((n_col, n_dev, half, d_cols), BF16),
            pltpu.VMEM((n_col, n_tp, half, d_cols), BF16),
            dma((n_gu,)), dma((n_gu,)), dma((n_dr,)), dma((n_sub,)), dma((n_sub,)), dma((7, n_sub)), dma((n_dev, n_sub)),
            dma((n_col, n_dev)), dma((n_col, n_dev)), dma((n_col,)), dma((n_col,)),
        ],
        compiler_params=pltpu.CompilerParams(
            collective_id=0, has_side_effects=True, vmem_limit_bytes=67043328),
        name="moe",
    )(part, hidden, b_out, ln_scale, ln_bias, w_router, ids_t, w_gate, w_up, w_down)


def solution(mesh):
    n_tp, n_ep = mesh.shape['tp'], mesh.shape['ep']
    token_rows = P(('dp', 'ep'), None)
    token_vec = P(('dp', 'ep'))
    cache_spec = P(('dp', 'ep'), None, 'tp', None)
    expert_in = P('ep', None, 'tp')
    expert_down = P('ep', 'tp', None)

    def device_step(hidden, seq_lens, rope_cos, rope_sin, ln1_scale, ln1_bias, w_qkv, b_qkv, w_out, b_out, k_cache, v_cache, ln2_scale, ln2_bias, w_router, expert_ids, w_gate, w_up, w_down):
        n_b, s_max, n_groups, head = k_cache.shape
        k_rows = k_cache.reshape(n_b, s_max * n_groups, head)
        v_rows = v_cache.reshape(n_b, s_max * n_groups, head)
        part, k_out, v_out = attention_call(
            hidden, seq_lens, rope_cos, rope_sin, ln1_scale, ln1_bias, w_qkv, b_qkv, w_out, k_rows, v_rows)
        hidden_out = moe_call(
            n_tp, n_ep, part, hidden, b_out, ln2_scale, ln2_bias, w_router, expert_ids.T, w_gate, w_up, w_down)
        return hidden_out, k_out.reshape(k_cache.shape), v_out.reshape(v_cache.shape)

    in_specs = (token_rows, token_vec, token_rows, token_rows, P(), P(), P(None, 'tp'), P('tp'), P('tp', None), P(), cache_spec, cache_spec, P(), P(), P(), token_rows, expert_in, expert_in, expert_down)
    return jax.shard_map(device_step, mesh=mesh, in_specs=in_specs, out_specs=(token_rows, cache_spec, cache_spec), check_vma=False)
```

```python
import functools

import jax
import jax.numpy as jnp
from jax import lax
from jax.experimental import pallas as pl
from jax.experimental.pallas import tpu as pltpu
from jax.sharding import PartitionSpec as P

EPS = 1e-5
F32 = jnp.float32
BF16 = jnp.bfloat16
MESH = pl.DeviceIdType.MESH
NT = (((1,), (1,)), ((), ()))


def as_row(vec):
    return vec.astype(F32).reshape(1, vec.shape[0])


def layer_norm(vals_f32, scale, bias):
    row_mean = jnp.mean(vals_f32, axis=-1, keepdims=True)
    centered = vals_f32 - row_mean
    row_var = jnp.mean(centered * centered, axis=-1, keepdims=True)
    normed = centered * lax.rsqrt(row_var + EPS)
    return (normed * as_row(scale) + as_row(bias)).astype(BF16)


def load_all(sources, targets, sems):
    copies = [pltpu.make_async_copy(src, dst, sems.at[i]) for i, (src, dst) in enumerate(zip(sources, targets))]
    for copy in copies:
        copy.start()
    return copies


def attn_kernel(seq_ref, hid_ref, cos_ref, sin_ref, lns_ref, lnb_ref, bq_ref, wq_hbm, kc_hbm, vc_hbm, wo_hbm,
                part_ref, ko_hbm, vo_hbm,
                wq_buf, kbuf, vbuf, wo_buf, hbuf, qs, ks, vs, ctx, cb,
                wq_sem, k_sem, v_sem, wo_sem, ko_sem, vo_sem):
    n_b = hid_ref.shape[0]
    n_wq, _, wq_cols = wq_buf.shape
    n_wo, _, wo_cols = wo_buf.shape
    rows = kbuf.shape[1]
    heads = qs.shape[0] // n_b
    chunk = 16
    n_chunk = n_b // chunk

    def wq_copy(n):
        return pltpu.make_async_copy(wq_hbm.at[:, pl.ds(n * wq_cols, wq_cols)], wq_buf.at[n], wq_sem.at[n])

    def k_copy(c):
        return pltpu.make_async_copy(kc_hbm.at[pl.ds(c * chunk, chunk)], kbuf.at[pl.ds(c * chunk, chunk)], k_sem.at[c])

    def v_copy(c):
        return pltpu.make_async_copy(vc_hbm.at[pl.ds(c * chunk, chunk)], vbuf.at[pl.ds(c * chunk, chunk)], v_sem.at[c])

    def wo_copy(n):
        return pltpu.make_async_copy(wo_hbm.at[:, pl.ds(n * wo_cols, wo_cols)], wo_buf.at[n], wo_sem.at[n])

    def ko_copy(c):
        return pltpu.make_async_copy(kbuf.at[pl.ds(c * chunk, chunk)], ko_hbm.at[pl.ds(c * chunk, chunk)], ko_sem.at[c])

    def vo_copy(c):
        return pltpu.make_async_copy(vbuf.at[pl.ds(c * chunk, chunk)], vo_hbm.at[pl.ds(c * chunk, chunk)], vo_sem.at[c])

    stages = [[] for _ in range(n_wq)]
    first = [wq_copy(n) for n in range(n_wq)] + [k_copy(0), v_copy(0)]
    for c in range(1, n_chunk):
        stages[min(c - 1, n_wq - 1)] += [k_copy(c), v_copy(c)]
    for n in range(n_wo):
        stages[min(n_chunk - 1 + n // 2, n_wq - 1)].append(wo_copy(n))
    for copy in first:
        copy.start()

    hbuf[...] = layer_norm(hid_ref[...].astype(F32), lns_ref[...], lnb_ref[...])
    cos2 = jnp.concatenate([cos_ref[...], cos_ref[...]], axis=1)
    sin2 = jnp.concatenate([-sin_ref[...], sin_ref[...]], axis=1)
    per_group = heads // 2 + 2
    for n in range(n_wq):
        wq_copy(n).wait()
        for copy in stages[n]:
            copy.start()
        cols = pl.ds(n * wq_cols, wq_cols)
        qkv = jnp.dot(hbuf[...], wq_buf[n], preferred_element_type=F32) + as_row(bq_ref[cols])
        qkv = qkv.astype(BF16).astype(F32)
        for i in range(wq_cols // 128):
            g, j = divmod(n * (wq_cols // 128) + i, per_group)
            block = qkv[:, i * 128:(i + 1) * 128]
            if j <= heads // 2:
                block = block * cos2 + pltpu.roll(block, 64, 1) * sin2
                block = block.astype(BF16).astype(F32)
            if j < heads // 2:
                qs[pl.ds(g * (heads // 2) + j, n_b, stride=heads), :] = block
            elif j == heads // 2:
                ks[pl.ds(g, n_b, stride=2), :] = block
            else:
                vs[pl.ds(g, n_b, stride=2), :] = block

    col = lax.broadcasted_iota(jnp.int32, (heads, rows), 1)
    head_row = lax.broadcasted_iota(jnp.int32, (heads, rows), 0)
    own_group = (col % 2) == (head_row // (heads // 2))
    position = jnp.where(own_group, col // 2, rows)
    tile_row = lax.broadcasted_iota(jnp.int32, (16, 128), 0)
    scale = 128 ** -0.5

    def one_chunk(c, _):
        k_copy(c).wait()
        v_copy(c).wait()
        lens = [seq_ref[c * chunk + i] for i in range(chunk)]
        for i in range(chunk):
            b = c * chunk + i
            base = pl.multiple_of((lens[i] // 8) * 16, 16)
            first = lens[i] * 2 - base
            for buf, new in ((kbuf, ks), (vbuf, vs)):
                tile = buf[b, pl.ds(base, 16), :].astype(F32)
                tile = jnp.where(tile_row == first, new[pl.ds(b * 2, 1), :], tile)
                tile = jnp.where(tile_row == first + 1, new[pl.ds(b * 2 + 1, 1), :], tile)
                buf[b, pl.ds(base, 16), :] = tile.astype(BF16)
        ko_copy(c).start()
        vo_copy(c).start()
        scores = []
        for i in range(chunk):
            b = c * chunk + i
            q = qs[pl.ds(pl.multiple_of(b * heads, heads), heads), :].astype(BF16)
            s = lax.dot_general(q, kbuf[b], NT, preferred_element_type=F32) * scale
            scores.append(jnp.where(position <= lens[i], s, -jnp.inf))
        probs = []
        for i in range(chunk):
            top = jnp.max(scores[i], axis=-1, keepdims=True)
            e = jnp.exp(scores[i] - top)
            probs.append((e / jnp.sum(e, axis=-1, keepdims=True)).astype(BF16))
        for i in range(chunk):
            b = c * chunk + i
            out = jnp.dot(probs[i], vbuf[b], preferred_element_type=F32)
            ctx[pl.ds(pl.multiple_of(b * heads, heads), heads), :] = out.astype(BF16).astype(F32)
        return 0

    lax.fori_loop(0, n_chunk, one_chunk, 0)
    for j in range(heads):
        cb[:, j * 128:(j + 1) * 128] = ctx[pl.ds(j, n_b, stride=heads), :].astype(BF16)
    for n in range(n_wo):
        wo_copy(n).wait()
        part_ref[:, pl.ds(n * wo_cols, wo_cols)] = jnp.dot(cb[...], wo_buf[n], preferred_element_type=F32).astype(BF16)
    for c in range(n_chunk):
        ko_copy(c).wait()
        vo_copy(c).wait()


def attention_call(hidden, seq_lens, rope_cos, rope_sin, ln_scale, ln_bias, w_qkv, b_qkv, w_out, k_rows, v_rows):
    n_b, d_model = hidden.shape
    heads = w_out.shape[0] // 128
    vmem = pl.BlockSpec(memory_space=pltpu.VMEM)
    hbm = pl.BlockSpec(memory_space=pl.ANY)
    wq_cols = 512
    wo_cols = 512
    n_wq = w_qkv.shape[1] // wq_cols
    n_wo = d_model // wo_cols
    dma = pltpu.SemaphoreType.DMA
    return pl.pallas_call(
        attn_kernel,
        out_shape=(
            pltpu.VMEM((n_b, d_model), BF16),
            jax.ShapeDtypeStruct(k_rows.shape, BF16),
            jax.ShapeDtypeStruct(v_rows.shape, BF16),
        ),
        in_specs=[pl.BlockSpec(memory_space=pltpu.SMEM)] + [vmem] * 6 + [hbm] * 4,
        out_specs=(vmem, hbm, hbm),
        scratch_shapes=[
            pltpu.VMEM((n_wq, d_model, wq_cols), BF16),
            pltpu.VMEM(k_rows.shape, BF16),
            pltpu.VMEM(v_rows.shape, BF16),
            pltpu.VMEM((n_wo, w_out.shape[0], wo_cols), BF16),
            pltpu.VMEM((n_b, d_model), BF16),
            pltpu.VMEM((n_b * heads, 128), F32),
            pltpu.VMEM((n_b * 2, 128), F32),
            pltpu.VMEM((n_b * 2, 128), F32),
            pltpu.VMEM((n_b * heads, 128), F32),
            pltpu.VMEM((n_b, heads * 128), BF16),
            dma((n_wq,)), dma((n_b // 16,)), dma((n_b // 16,)), dma((n_wo,)), dma((n_b // 16,)), dma((n_b // 16,)),
        ],
        compiler_params=pltpu.CompilerParams(vmem_limit_bytes=60 * 1024 * 1024),
        name="attn",
    )(seq_lens, hidden, rope_cos, rope_sin, ln_scale, ln_bias, b_qkv, w_qkv, k_rows, v_rows, w_out)


def moe_kernel(n_tp, n_ep, part_ref, hid_in, bout_in, lns_in, lnb_in, wr_in, ids_in, wg_hbm, wu_hbm, wd_hbm,
               out_ref,
               hid_ref, bout_ref, lns_ref, lnb_ref, wr_ref, ids_ref, in_sem,
               ring, hall, arx, x1buf, dmat, cmat, xbuf, abuf, ybuf, pbuf, rbuf, obuf,
               gu_sem, d_sem, a_send, a_recv, h_send, h_recv, r_send, r_recv, o_send, o_recv):
    me_t = lax.axis_index("tp")
    me_e = lax.axis_index("ep")
    n_dev = n_tp * n_ep
    me = me_e * n_tp + me_t
    n_slot, d_rows, d_cols = ring.shape
    d_model, width = wg_hbm.shape[1:]
    edge = width - d_cols
    d_group = d_rows // width
    n_local = wg_hbm.shape[0]
    n_exp = n_local * n_ep
    half = x1buf.shape[0]
    shard = half * n_tp
    n_rows = hall.shape[0]
    cap = 32
    n_col = d_model // d_cols
    n_grp = n_local // d_group
    n_down = n_col * n_grp
    x_group = xbuf.shape[0] // cap
    n_xg = n_local // x_group
    n_unroll = 4

    def peer_of(d):
        pid = lax.rem(me + d, n_dev)
        return pid, {"tp": lax.rem(pid, n_tp), "ep": lax.div(pid, n_tp)}

    def gu_copies(i):
        slot = lax.rem(i, n_slot)
        top, mid, low = (pl.ds(n * d_model, d_model) for n in range(3))
        left, right = pl.ds(0, edge), pl.ds(edge, edge)
        pieces = (
            (wg_hbm.at[i, :, pl.ds(0, d_cols)], ring.at[slot, top]),
            (wg_hbm.at[i, :, pl.ds(d_cols, edge)], ring.at[slot, mid, left]),
            (wu_hbm.at[i, :, pl.ds(0, edge)], ring.at[slot, mid, right]),
            (wu_hbm.at[i, :, pl.ds(edge, d_cols)], ring.at[slot, low]))
        return [pltpu.make_async_copy(src, dst, gu_sem.at[slot, n]) for n, (src, dst) in enumerate(pieces)]

    def d_copy(q):
        slot = lax.rem(n_local + q, n_slot)
        grp = lax.rem(q, n_grp)
        col = lax.div(q, n_grp)
        src = wd_hbm.at[pl.ds(pl.multiple_of(grp * d_rows, d_rows), d_rows),
                        pl.ds(pl.multiple_of(col * d_cols, d_cols), d_cols)]
        return pltpu.make_async_copy(src, ring.at[slot], d_sem.at[slot])

    def start_gu(i, _=0):
        for copy in gu_copies(i):
            copy.start()
        return 0

    barrier = pltpu.get_barrier_semaphore()
    for d in range(1, n_dev):
        _, dev = peer_of(d)
        pl.semaphore_signal(barrier, inc=1, device_id=dev, device_id_type=MESH)
    small = load_all((hid_in, bout_in, lns_in, lnb_in, wr_in, ids_in),
                     (hid_ref, bout_ref, lns_ref, lnb_ref, wr_ref, ids_ref), in_sem)
    lax.fori_loop(0, n_slot, start_gu, 0)
    for copy in small:
        copy.wait()
    pl.semaphore_wait(barrier, n_dev - 1)

    other_t = 1 - me_t
    core = lax.rem(me_e, 2)
    sib_e = me_e + 1 - 2 * core
    far_e = lax.rem(me_e + 2, n_ep)
    near_dev = {"tp": me_t, "ep": sib_e}
    n_sub = a_send.shape[0]
    sub = half // n_sub

    def a_copy(s):
        rows = pl.ds(pl.multiple_of(other_t * half + s * sub, sub), sub)
        return pltpu.make_async_remote_copy(
            src_ref=part_ref.at[rows], dst_ref=arx.at[pl.ds(s * sub, sub)], send_sem=a_send.at[s],
            recv_sem=a_recv.at[s], device_id={"tp": other_t, "ep": me_e}, device_id_type=MESH)

    for s in range(n_sub):
        a_copy(s).start()

    def h_copy(step, s, block_e, block_t, dev):
        block = block_e * n_tp + block_t
        rows = pl.ds(pl.multiple_of(block * half + s * sub, sub), sub)
        return pltpu.make_async_remote_copy(
            src_ref=hall.at[rows], dst_ref=hall.at[rows], send_sem=h_send.at[step, s], recv_sem=h_recv.at[block, s],
            device_id=dev, device_id_type=MESH)

    far_dev = {"tp": me_t, "ep": far_e}
    side_dev = {"tp": other_t, "ep": me_e}
    diag_dev = {"tp": other_t, "ep": far_e}
    sends = (
        (0, me_e, me_t, far_dev), (1, me_e, me_t, side_dev), (2, me_e, me_t, near_dev), (3, me_e, me_t, diag_dev),
        (4, far_e, me_t, near_dev), (5, me_e, other_t, near_dev), (6, far_e, other_t, near_dev))

    picked_t = jnp.zeros((n_exp, shard), F32)
    exp_row = lax.broadcasted_iota(jnp.int32, (n_exp, shard), 0)
    for k in range(ids_ref.shape[0]):
        picked_t = picked_t + (exp_row == ids_ref[pl.ds(k, 1), :]).astype(F32)
    sel = (lax.broadcasted_iota(jnp.int32, (half, shard), 1)
           == lax.broadcasted_iota(jnp.int32, (half, shard), 0) + me_t * half).astype(BF16)
    picked = lax.dot_general(sel, picked_t.astype(BF16), NT, preferred_element_type=F32)

    my_rows = pl.ds(pl.multiple_of(me * half, half), half)
    for s in range(n_sub):
        rows = pl.ds(pl.multiple_of(me_t * half + s * sub, sub), sub)
        attn = part_ref[rows, :].astype(F32)
        base = hid_ref[rows, :].astype(F32)
        a_copy(s).wait_recv()
        attn = attn + arx[s * sub:(s + 1) * sub, :].astype(F32)
        x1 = (base + attn + as_row(bout_ref[...])).astype(BF16)
        x1buf[s * sub:(s + 1) * sub, :] = x1
        h2 = layer_norm(x1.astype(F32), lns_ref[...], lnb_ref[...])
        hall_rows = pl.ds(pl.multiple_of(me * half + s * sub, sub), sub)
        hall[hall_rows, pl.ds(0, d_model)] = h2
        logits = jnp.dot(h2, wr_ref[...], preferred_element_type=F32)
        logits = jnp.where(picked[s * sub:(s + 1) * sub, :] > 0.5, logits, -jnp.inf)
        e = jnp.exp(logits - jnp.max(logits, axis=-1, keepdims=True))
        gates = e / jnp.sum(e, axis=-1, keepdims=True)
        hall[hall_rows, pl.ds(d_model, n_exp)] = gates.astype(BF16)
        for step, block_e, block_t, dev in sends[:4]:
            h_copy(step, s, block_e, block_t, dev).start()

    for s in range(n_sub):
        for step, block_e, block_t, dev in sends[4:]:
            h_copy(0, s, block_e, block_t, near_dev).wait_recv()
            h_copy(step, s, block_e, block_t, dev).start()
    for s in range(n_sub):
        for block_e, block_t in ((sib_e, me_t), (sib_e, other_t), (lax.rem(sib_e + 2, n_ep), me_t),
                                 (lax.rem(sib_e + 2, n_ep), other_t)):
            h_copy(0, s, block_e, block_t, near_dev).wait_recv()

    gate_cols = pl.ds(d_model, n_exp)
    pick = (lax.broadcasted_iota(jnp.int32, (n_local, n_exp), 1)
            == lax.broadcasted_iota(jnp.int32, (n_local, n_exp), 0) + me_e * n_local).astype(BF16)
    row_i = lax.broadcasted_iota(jnp.int32, (n_rows, n_rows), 0)
    col_i = lax.broadcasted_iota(jnp.int32, (n_rows, n_rows), 1)
    same = (row_i // shard) == (col_i // shard)

    gate_t = lax.dot_general(pick, hall[:, gate_cols], NT, preferred_element_type=F32)
    upper = jnp.where((row_i < col_i) & same, 1.0, 0.0).astype(BF16)
    rank_t = jnp.dot(jnp.where(gate_t > 0, 1.0, 0.0).astype(BF16), upper, preferred_element_type=F32)
    shard_t = (lax.broadcasted_iota(jnp.int32, (n_local, n_rows), 1) // shard * (cap // n_ep)).astype(F32)
    key_t = jnp.where(gate_t > 0, rank_t + shard_t, -1.0)
    slot_i = lax.broadcasted_iota(jnp.int32, (cap, n_rows), 0).astype(F32)
    for i in range(n_local):
        dmat[i * cap:(i + 1) * cap, :] = jnp.where(key_t[i:i + 1, :] == slot_i, 1.0, 0.0).astype(BF16)

    def expert_group(g, _):
        rows = pl.ds(pl.multiple_of(g * x_group * cap, x_group * cap), x_group * cap)
        for c in range(4):
            cols = pl.ds(c * (d_model // 4), d_model // 4)
            xbuf[:, cols] = jnp.dot(dmat[rows, :], hall[:, cols], preferred_element_type=F32).astype(BF16)

        def some_experts(k, _):
            first = g * x_group + k * n_unroll
            for u in range(n_unroll):
                for copy in gu_copies(first + u):
                    copy.wait()
            parts = []
            for u in range(n_unroll):
                slot = lax.rem(first + u, n_slot)
                x = xbuf[pl.ds(pl.multiple_of((k * n_unroll + u) * cap, cap), cap), :]
                parts.append([jnp.dot(x, ring[slot, n * d_model:(n + 1) * d_model, :], preferred_element_type=F32)
                              for n in range(3)])
            for u in range(n_unroll):
                top, mid, low = parts[u]
                gate_pre = jnp.concatenate([top, mid[:, :edge]], axis=1)
                up_pre = jnp.concatenate([mid[:, edge:], low], axis=1)
                act = (gate_pre * jax.nn.sigmoid(gate_pre) * up_pre).astype(BF16)
                abuf[pl.ds(pl.multiple_of((first + u) * cap, cap), cap), :] = act
            for u in range(n_unroll):
                item = first + u + n_slot

                @pl.when(item < n_local)
                def _():
                    start_gu(item)

                @pl.when((item >= n_local) & (item < n_local + n_down))
                def _():
                    d_copy(item - n_local).start()

            return 0

        lax.fori_loop(0, x_group // n_unroll, some_experts, 0)
        return 0

    lax.fori_loop(0, n_xg - 1, expert_group, 0)

    gate_l = lax.dot_general(hall[:, gate_cols], pick, NT, preferred_element_type=F32)
    lower = jnp.where((row_i > col_i) & same, 1.0, 0.0).astype(BF16)
    rank_l = jnp.dot(lower, jnp.where(gate_l > 0, 1.0, 0.0).astype(BF16), preferred_element_type=F32)
    shard_l = (lax.broadcasted_iota(jnp.int32, (n_rows, n_local), 0) // shard * (cap // n_ep)).astype(F32)
    key_l = jnp.where(gate_l > 0, rank_l + shard_l, -1.0).astype(BF16)
    gate_b = gate_l.astype(BF16)
    step = 256
    for c in range(n_local * cap // step):
        spread = (lax.broadcasted_iota(jnp.int32, (n_local, step), 0)
                  == (lax.broadcasted_iota(jnp.int32, (n_local, step), 1) + c * step) // cap).astype(BF16)
        key_x = jnp.dot(key_l, spread, preferred_element_type=F32)
        gate_x = jnp.dot(gate_b, spread, preferred_element_type=F32)
        lane = (lax.broadcasted_iota(jnp.int32, (n_rows, step), 1) % cap).astype(F32)
        cmat[:, pl.ds(c * step, step)] = jnp.where(key_x == lane, gate_x, 0.0).astype(BF16)

    lax.fori_loop(n_xg - 1, n_xg, expert_group, 0)

    def r_copy(j, d, block_sent, block_from, dev):
        rows = pl.ds(pl.multiple_of(block_sent * half, half), half)
        return pltpu.make_async_remote_copy(
            src_ref=pbuf.at[j, rows], dst_ref=rbuf.at[j, block_from], send_sem=r_send.at[j, d],
            recv_sem=r_recv.at[j, block_from], device_id=dev, device_id_type=MESH)

    def o_copy(j, block_t):
        return pltpu.make_async_remote_copy(
            src_ref=obuf.at[j, block_t], dst_ref=obuf.at[j, block_t], send_sem=o_send.at[j], recv_sem=o_recv.at[j],
            device_id={"tp": other_t, "ep": me_e}, device_id_type=MESH)

    def finish(j):
        cols = pl.ds(pl.multiple_of(j * d_cols, d_cols), d_cols)
        total = pbuf[j, my_rows, :].astype(F32)
        for d in range(1, n_dev):
            pid, dev = peer_of(d)
            r_copy(j, d, pid, pid, dev).wait_recv()
            total = total + rbuf[j, pid].astype(F32)
        obuf[j, me_t] = (x1buf[:, cols].astype(F32) + total).astype(BF16)
        o_copy(j, me_t).start()

    lag = 2

    def one_col(j, _):
        def one_part(g, _):
            q = j * n_grp + g
            slot = lax.rem(n_local + q, n_slot)
            main = width - edge
            pad = jnp.zeros((cap, edge), BF16)
            for k in range(0, d_group, 2):
                rows = [pl.ds(pl.multiple_of((g * d_group + k + u) * cap, cap), cap) for u in range(2)]
                acts = [abuf[rows[u], :] for u in range(2)]
                ends = jnp.concatenate([
                    jnp.concatenate([acts[0][:, main:], pad], axis=1),
                    jnp.concatenate([pad, acts[1][:, main:]], axis=1)], axis=0)
                end_w = jnp.concatenate([ring[slot, (k + u) * width + main:(k + u + 1) * width, :] for u in range(2)], axis=0)
                tail = jnp.dot(ends, end_w, preferred_element_type=F32)
                for u in range(2):
                    top = (k + u) * width
                    y = jnp.dot(acts[u][:, :main], ring[slot, top:top + main, :], preferred_element_type=F32)
                    ybuf[rows[u], :] = (y + tail[u * cap:(u + 1) * cap]).astype(BF16)

            @pl.when(q + n_slot < n_down)
            def _():
                d_copy(q + n_slot).start()

            return 0

        for g in range(n_grp):
            d_copy(j * n_grp + g).wait()
        for g in range(n_grp):
            one_part(g, 0)
        for u in range(2):
            part_rows = slice(u * n_rows // 2, (u + 1) * n_rows // 2)
            pbuf[j, part_rows, :] = jnp.dot(cmat[part_rows, :], ybuf[...], preferred_element_type=F32).astype(BF16)
        for d in range(1, n_dev):
            pid, dev = peer_of(d)
            r_copy(j, d, pid, me, dev).start()

        @pl.when(j >= lag)
        def _():
            finish(j - lag)

        return 0

    lax.fori_loop(0, n_col, one_col, 0)
    for j in range(n_col - lag, n_col):
        finish(j)

    def drain(j, _):
        for d in range(1, n_dev):
            pid, dev = peer_of(d)
            r_copy(j, d, pid, me, dev).wait_send()
        o_copy(j, me_t).wait_send()
        return 0

    lax.fori_loop(0, n_col, drain, 0)
    for s in range(n_sub):
        a_copy(s).wait_send()
        for step, block_e, block_t, dev in sends:
            h_copy(step, s, block_e, block_t, dev).wait_send()
    for j in range(n_col):
        o_copy(j, other_t).wait_recv()
        for t in range(n_tp):
            out_ref[t * half:(t + 1) * half, j * d_cols:(j + 1) * d_cols] = obuf[j, t]


def moe_call(n_tp, n_ep, part, hidden, b_out, ln_scale, ln_bias, w_router, ids_t, w_gate, w_up, w_down):
    n_b, d_model = hidden.shape
    n_local, _, width = w_gate.shape
    n_exp = n_local * n_ep
    n_rows = n_b * n_ep
    n_dev = n_tp * n_ep
    half = n_b // n_tp
    cap = 32
    n_slot, d_cols = 16, 256
    n_sub = 2
    n_col = d_model // d_cols
    vmem = pl.BlockSpec(memory_space=pltpu.VMEM)
    hbm = pl.BlockSpec(memory_space=pl.ANY)
    dma = pltpu.SemaphoreType.DMA
    return pl.pallas_call(
        functools.partial(moe_kernel, n_tp, n_ep),
        out_shape=pltpu.VMEM((n_b, d_model), BF16),
        in_specs=[vmem] + [hbm] * 9,
        out_specs=vmem,
        scratch_shapes=[pltpu.VMEM(x.shape, x.dtype) for x in (hidden, b_out, ln_scale, ln_bias, w_router, ids_t)] + [
            dma((6,)),
            pltpu.VMEM((n_slot, 3 * d_model, d_cols), BF16),
            pltpu.VMEM((n_rows, d_model + n_exp), BF16),
            pltpu.VMEM((half, d_model), BF16),
            pltpu.VMEM((half, d_model), BF16),
            pltpu.VMEM((n_local * cap, n_rows), BF16),
            pltpu.VMEM((n_rows, n_local * cap), BF16),
            pltpu.VMEM((8 * cap, d_model), BF16),
            pltpu.VMEM((n_local * cap, width), BF16),
            pltpu.VMEM((n_local * cap, d_cols), BF16),
            pltpu.VMEM((n_col, n_rows, d_cols), BF16),
            pltpu.VMEM((n_col, n_dev, half, d_cols), BF16),
            pltpu.VMEM((n_col, n_tp, half, d_cols), BF16),
            dma((n_slot, 4)), dma((n_slot,)), dma((n_sub,)), dma((n_sub,)), dma((7, n_sub)), dma((n_dev, n_sub)),
            dma((n_col, n_dev)), dma((n_col, n_dev)), dma((n_col,)), dma((n_col,)),
        ],
        compiler_params=pltpu.CompilerParams(
            collective_id=0, has_side_effects=True, vmem_limit_bytes=65700000),
        name="moe",
    )(part, hidden, b_out, ln_scale, ln_bias, w_router, ids_t, w_gate, w_up, w_down)


def solution(mesh):
    n_tp, n_ep = mesh.shape['tp'], mesh.shape['ep']
    token_rows = P(('dp', 'ep'), None)
    token_vec = P(('dp', 'ep'))
    cache_spec = P(('dp', 'ep'), None, 'tp', None)
    expert_in = P('ep', None, 'tp')
    expert_down = P('ep', 'tp', None)

    def device_step(hidden, seq_lens, rope_cos, rope_sin, ln1_scale, ln1_bias, w_qkv, b_qkv, w_out, b_out, k_cache, v_cache, ln2_scale, ln2_bias, w_router, expert_ids, w_gate, w_up, w_down):
        n_b, s_max, n_groups, head = k_cache.shape
        k_rows = k_cache.reshape(n_b, s_max * n_groups, head)
        v_rows = v_cache.reshape(n_b, s_max * n_groups, head)
        part, k_out, v_out = attention_call(
            hidden, seq_lens, rope_cos, rope_sin, ln1_scale, ln1_bias, w_qkv, b_qkv, w_out, k_rows, v_rows)
        part = pltpu.with_memory_space_constraint(part, pltpu.VMEM)
        hidden_out = moe_call(
            n_tp, n_ep, part, hidden, b_out, ln2_scale, ln2_bias, w_router, expert_ids.T, w_gate, w_up,
            w_down.reshape(-1, w_down.shape[2]))
        return hidden_out, k_out.reshape(k_cache.shape), v_out.reshape(v_cache.shape)

    in_specs = (token_rows, token_vec, token_rows, token_rows, P(), P(), P(None, 'tp'), P('tp'), P('tp', None), P(), cache_spec, cache_spec, P(), P(), P(), token_rows, expert_in, expert_in, expert_down)
    return jax.shard_map(device_step, mesh=mesh, in_specs=in_specs, out_specs=(token_rows, cache_spec, cache_spec), check_vma=False)
```
